32 devices in a mesh: freq: 4 (over y, x), band: 8 (over z, core).
Axes of the slice: x: 2, y: 2, z: 4, core: 2. Of those that a mesh axis runs over, the one named last changes fastest.
Arguments:
- pair_density: bfloat16 [1024, 2, 8192], P(('freq', 'band')), may hold values from -6 to 6
- trial_vectors: bfloat16 [16, 2, 64, 8192], P('freq', None, None, 'band'), may hold values from -6 to 6
- frequency: float32 [16], P('freq'), may hold values from 0.05 to 20
- val_energy: float32 [32], replicated, may hold values from -3 to -0.1
- cond_energy: float32 [32], replicated, may hold values from 0.1 to 4
- pair_index: int32 [1024], P(('freq', 'band')), may hold values from 0 to 1023, each once
Outputs:
- images: float32 [16, 2, 64, 8192], P('freq', None, None, 'band')
- subspace: float32 [16, 2, 64, 64], P('freq')
The draws below stay inside these ranges and needn't reach their ends.
Inputs may be any that keep to these rules, and one draw needn't show every extreme that they name: `pair_index`: every pair number 0 to 1023 appears exactly once.
All inputs are finite; a program needn't handle non-finite values.
Results may differ from the reference program's by a relative error of at most 0.0085.
Values may be sent and summed in bfloat16 or wider, within the bound.
No kernel may reach another device: no remote copies, remote signals or barrier semaphores. Data moves between devices by JAX's collectives and lax.ppermute only.
A program may use at most 128 MiB of HBM per device.

```python
import math
import jax
import jax.numpy as jnp
from jax import lax

NG = 8192
NV = 32
K = 64
NFREQ = 16
PAIRS = 1024
NC = 32


def block_scale(own_key, dims, shards, smallest, top_value):
    gain = 1.0
    for position, shards_of in shards:
        draws = jax.random.uniform(jax.random.fold_in(jax.random.fold_in(own_key, 6), position), (shards_of,), jnp.float32, smallest / len(shards), top_value / len(shards))
        gain = gain * jnp.repeat(jnp.exp(draws), dims[position] // shards_of).reshape((-1,) + (1,) * (len(dims) - 1 - position))
    return gain


def bell_draw(rng, extent, spread, most, shards=(), kind=jnp.bfloat16):
    loudness = block_scale(rng, extent, shards, -0.22, 0.18) if shards else 1.0
    array = jax.random.normal(rng, extent, jnp.float32) * spread * loudness
    return jnp.minimum(jnp.maximum(array, -most), most).astype(kind)


def setup_inputs(seed: int = 0) -> dict:
    keys = jax.random.split(jax.random.key(seed), 7)
    pair_density = bell_draw(keys[0], (PAIRS, 2, NG), 1.0, 6.0, ((0, 32),))
    trial_vectors = bell_draw(keys[1], (NFREQ, 2, K, NG), 1.0, 6.0, ((0, 4), (3, 8)))
    frequency = jnp.clip(jnp.exp(math.log(20.0) - 5.9914645 * jax.random.uniform(keys[2], (NFREQ,), jnp.float32) ** block_scale(keys[2], (NFREQ,), ((0, 4),), -0.2, 0.2)), 0.05, 20.0)
    val_energy = jnp.clip(jax.random.uniform(keys[3], (NV,), jnp.float32, -3.0, -0.1), -3.0, -0.1)
    cond_energy = jnp.clip(jax.random.uniform(keys[4], (NC,), jnp.float32, 0.1, 4.0), 0.1, 4.0)
    pair_index = jax.random.permutation(keys[5], PAIRS).astype(jnp.int32)
    return dict(pair_density=pair_density, trial_vectors=trial_vectors, frequency=frequency, val_energy=val_energy, cond_energy=cond_energy, pair_index=pair_index)


def pair_weights(pair_index, frequency, val_energy, cond_energy):
    delta = cond_energy[pair_index % NC] - val_energy[pair_index // NC]
    prefactor = 1.0 / math.sqrt(2.0 * NG * PAIRS)
    ratio = delta[None, :] / (delta[None, :] * delta[None, :] + frequency[:, None] * frequency[:, None])
    return (-4.0 * prefactor * ratio).astype(jnp.bfloat16)

def reference(pair_density, trial_vectors, frequency, val_energy, cond_energy, pair_index):
    density = pair_density.astype(jnp.float32)
    vectors = trial_vectors.astype(jnp.float32)
    weight = pair_weights(pair_index, frequency, val_energy, cond_energy).astype(jnp.float32)
    products = jnp.einsum('pcg,fekg->fcekp', density, vectors)
    over_real = products[:, 0, 0] + products[:, 1, 1]
    over_imag = products[:, 0, 1] - products[:, 1, 0]
    scaled_real = (weight[:, None, :] * over_real).astype(jnp.bfloat16)
    scaled_imag = (weight[:, None, :] * over_imag).astype(jnp.bfloat16)
    mixed = jnp.stack([jnp.stack([scaled_real, -scaled_imag], 1), jnp.stack([scaled_imag, scaled_real], 1)], 1)
    images = jnp.einsum('pcg,fdckp->fdkg', density, mixed.astype(jnp.float32))
    hp = lax.Precision.HIGHEST
    real_part = jnp.einsum('fkg,flg->fkl', vectors[:, 0], images[:, 0], precision=hp) + jnp.einsum('fkg,flg->fkl', vectors[:, 1], images[:, 1], precision=hp)
    imag_part = jnp.einsum('fkg,flg->fkl', vectors[:, 0], images[:, 1], precision=hp) - jnp.einsum('fkg,flg->fkl', vectors[:, 1], images[:, 0], precision=hp)
    subspace = jnp.stack([real_part, imag_part], 1) / NG
    return (images, subspace)
```

```python
import functools
import math

import jax
import jax.numpy as jnp
from jax import lax
from jax.experimental import pallas as pl
from jax.experimental.pallas import tpu as pltpu
from jax.sharding import PartitionSpec as P

CHUNKS = 2
VMEM = pltpu.VMEM


def split_kernel(rows, density_ref, *out_refs):
    block = density_ref[...].astype(jnp.float32)
    for part in range(2):
        values = block[:, part, :].astype(jnp.bfloat16)
        for chunk, out_ref in enumerate(out_refs):
            out_ref[0, part * rows : (part + 1) * rows, :] = values[chunk * rows : (chunk + 1) * rows]


def split_density(pair_density, members):
    stored, _, grid_all = pair_density.shape
    grid_own = grid_all // members
    rows = stored // CHUNKS
    return pl.pallas_call(
        functools.partial(split_kernel, rows),
        grid=(members,),
        in_specs=[pl.BlockSpec((stored, 2, grid_own), lambda b: (0, 0, b))],
        out_specs=[pl.BlockSpec((1, 2 * rows, grid_own), lambda b: (b, 0, 0))] * CHUNKS,
        out_shape=[jax.ShapeDtypeStruct((members, 2 * rows, grid_own), jnp.bfloat16)] * CHUNKS,
        name="split_density",
    )(pair_density)


def flip(value, axis, size, mask):
    return lax.ppermute(value, axis, [(i, i ^ mask) for i in range(size)])


def gather_groups(first, second, groups):
    first_parts, second_parts = {0: first}, {0: second}
    for mask in range(1, groups):
        low = mask & -mask
        high = 1 << (mask.bit_length() - 1)
        first_parts[mask] = flip(first_parts[mask ^ high], "freq", groups, high)
        second_parts[mask] = flip(second_parts[mask ^ low], "freq", groups, low)
    return [(first_parts[mask], second_parts[mask]) for mask in range(groups)]


def part_rows(refs, part, rows):
    blocks = []
    for ref in refs:
        block = ref[:, part * rows : (part + 1) * rows, :]
        blocks.append(block.reshape(block.shape[0] * rows, block.shape[2]))
    return jnp.concatenate(blocks, 0)


def crossing_kernel(groups, rows, core_ref, vectors_ref, *refs):
    density_refs, (out_ref,) = refs[: 2 * groups], refs[2 * groups :]
    freqs, _, vecs, grid_own = vectors_ref.shape
    half = out_ref.shape[1]
    share = out_ref.shape[3]
    pieces = vecs // share
    core = core_ref[0]
    vectors = vectors_ref[...].reshape(freqs * 2 * vecs, grid_own)
    for group in range(groups):
        pair = density_refs[2 * group : 2 * group + 2]
        products = []
        for part in range(2):
            density = part_rows(pair, part, rows)
            product = lax.dot_general(
                vectors, density, (((1,), (1,)), ((), ())), preferred_element_type=jnp.float32
            )
            products.append(product.reshape(freqs, 2, vecs, density.shape[0]))
        width = products[0].shape[3]
        columns = slice(group * width, (group + 1) * width)
        terms = (
            (products[0][:, 0] + products[1][:, 1]).astype(jnp.bfloat16),
            (products[0][:, 1] - products[1][:, 0]).astype(jnp.bfloat16),
        )
        for part in range(2):
            for f in range(freqs):
                for piece in range(pieces):
                    member = f * pieces + piece
                    out_ref[(member % 2) ^ core, member // 2, part, :, columns] = terms[part][
                        f, piece * share : (piece + 1) * share
                    ]


def partial_crossings(core, vectors, density, members, rows):
    groups = len(density)
    freqs, _, vecs, grid_own = vectors.shape
    share = freqs * vecs // members
    width = members * rows * groups
    flat = [block for pair in density for block in pair]
    return pl.pallas_call(
        functools.partial(crossing_kernel, groups, rows),
        in_specs=[pl.BlockSpec(memory_space=pltpu.SMEM)] + [pl.BlockSpec(memory_space=VMEM)] * (1 + len(flat)),
        out_specs=pl.BlockSpec(memory_space=VMEM),
        out_shape=jax.ShapeDtypeStruct((2, members // 2, 2, share, width), jnp.bfloat16),
        cost_estimate=pl.CostEstimate(
            flops=8 * freqs * vecs * grid_own * width, bytes_accessed=4 << 20, transcendentals=0
        ),
        name="partial_crossings",
    )(core, vectors, *flat)


def image_kernel(groups, rows, grid_count, core_ref, weights_ref, *refs):
    scaled_refs, refs = refs[: 2 * CHUNKS], refs[2 * CHUNKS :]
    density_refs = refs[: 2 * groups * CHUNKS]
    images_ref, subspace_ref, scaled_scr = refs[2 * groups * CHUNKS :]
    freqs, _, vecs, _ = images_ref.shape
    members_half, _, share, width = scaled_refs[0].shape
    pieces = vecs // share

    @pl.when(pl.program_id(0) == 0)
    def _():
        core = core_ref[0]
        for chunk in range(CHUNKS):
            own, other = scaled_refs[2 * chunk : 2 * chunk + 2]
            for member in range(2 * members_half):
                f, piece = member // pieces, member % pieces
                mine = core == member % 2
                for part in range(2):
                    row = (f * 2 + part) * vecs + piece * share
                    value = jnp.where(
                        mine,
                        own[member // 2, part].astype(jnp.float32),
                        other[member // 2, part].astype(jnp.float32),
                    )
                    scaled_scr[row : row + share, chunk * width : (chunk + 1) * width] = value.astype(
                        jnp.bfloat16
                    )
        for f in range(freqs):
            rows_f = scaled_scr[f * 2 * vecs : (f + 1) * 2 * vecs, :]
            ratio = rows_f.astype(jnp.float32) / weights_ref[f : f + 1, :]
            high = ratio.astype(jnp.bfloat16)
            low = (ratio - high.astype(jnp.float32)).astype(jnp.bfloat16)
            dims = (((1,), (1,)), ((), ()))
            gram = lax.dot_general(high, rows_f, dims, preferred_element_type=jnp.float32)
            gram += lax.dot_general(low, rows_f, dims, preferred_element_type=jnp.float32)
            gram = gram * (1.0 / grid_count)
            subspace_ref[f, 0] = gram[:vecs, :vecs] + gram[vecs:, vecs:]
            subspace_ref[f, 1] = gram[:vecs, vecs:] - gram[vecs:, :vecs]

    scaled = scaled_scr[...]
    products = []
    for part in range(2):
        density = jnp.concatenate(
            [part_rows(density_refs[2 * n : 2 * n + 2], part, rows) for n in range(groups * CHUNKS)], 0
        )
        product = jnp.dot(scaled, density, preferred_element_type=jnp.float32)
        products.append(product.reshape(freqs, 2, vecs, product.shape[1]))
    images_ref[:, 0] = products[0][:, 0] - products[1][:, 1]
    images_ref[:, 1] = products[0][:, 1] + products[1][:, 0]


def make_images(core, weights, scaled, density, freqs, vecs, rows, groups, grid_count):
    flat_scaled = [s for pair in scaled for s in pair]
    flat = [block for chunk in density for pair in chunk for block in pair]
    grid_own = flat[0].shape[2]
    tile = math.gcd(grid_own, 256)
    total = weights.shape[1]
    whole = pl.BlockSpec(memory_space=VMEM)
    return pl.pallas_call(
        functools.partial(image_kernel, groups, rows, grid_count),
        grid=(grid_own // tile,),
        in_specs=[pl.BlockSpec(memory_space=pltpu.SMEM), whole]
        + [whole] * len(flat_scaled)
        + [pl.BlockSpec(flat[0].shape[:2] + (tile,), lambda t: (0, 0, t))] * len(flat),
        out_specs=[
            pl.BlockSpec((freqs, 2, vecs, tile), lambda t: (0, 0, 0, t)),
            pl.BlockSpec((freqs, 2, vecs, vecs), lambda t: (0, 0, 0, 0)),
        ],
        out_shape=[
            jax.ShapeDtypeStruct((freqs, 2, vecs, grid_own), jnp.float32),
            jax.ShapeDtypeStruct((freqs, 2, vecs, vecs), jnp.float32),
        ],
        scratch_shapes=[VMEM((freqs * 2 * vecs, total), jnp.bfloat16)],
        name="make_images",
    )(core, weights, *flat_scaled, *flat)


def pair_weights(pair_index, frequency, val_energy, cond_energy, prefactor):
    cond_count = cond_energy.shape[0]
    val_count = val_energy.shape[0]
    cond_pick = jnp.sum(
        jnp.where(
            jnp.arange(cond_count)[:, None] == (pair_index % cond_count)[None, :], cond_energy[:, None], 0.0
        ),
        axis=0,
    )
    val_pick = jnp.sum(
        jnp.where(
            jnp.arange(val_count)[:, None] == (pair_index // cond_count)[None, :], val_energy[:, None], 0.0
        ),
        axis=0,
    )
    delta = cond_pick - val_pick
    ratio = delta[None, :] / (
        delta[None, :] * delta[None, :] + frequency[:, None] * frequency[:, None]
    )
    return lax.reduce_precision(-4.0 * prefactor * ratio, 8, 7)


def all_pair_numbers(pair_index, groups, members):
    me = lax.axis_index("band")
    slots = jnp.where(jnp.arange(members)[:, None] == me, pair_index[None, :], 0)
    mask = 1
    while mask < members:
        slots = slots + flip(slots, "band", members, mask)
        mask *= 2
    parts = [slots] + [flip(slots, "freq", groups, mask) for mask in range(1, groups)]
    rows = pair_index.shape[0] // CHUNKS
    blocks = [part[:, c * rows : (c + 1) * rows].reshape(-1) for c in range(CHUNKS) for part in parts]
    return jnp.concatenate(blocks)


def shards(pair_density, trial_vectors, frequency, val_energy, cond_energy, pair_index):
    groups = lax.axis_size("freq")
    members = lax.axis_size("band")
    stored = pair_density.shape[0]
    rows = stored // CHUNKS
    freqs, _, vecs, grid_own = trial_vectors.shape
    pair_count = stored * groups * members
    grid_count = grid_own * members
    prefactor = 1.0 / math.sqrt(2.0 * grid_count * pair_count)
    share = freqs * vecs // members
    pieces = vecs // share
    width = members * rows * groups
    me = lax.axis_index("band")
    core = (me % 2).astype(jnp.int32).reshape(1)
    lines = [[2 * z + c for z in range(members // 2)] for c in range(2)]

    numbers = all_pair_numbers(pair_index, groups, members)
    weights = pair_weights(numbers, frequency, val_energy, cond_energy, prefactor)
    own_weights = lax.dynamic_slice_in_dim(weights, me // pieces, 1, 0)

    density, partial = [], []
    for packed in split_density(pair_density, members):
        swapped = lax.all_to_all(packed, "band", split_axis=0, concat_axis=0, tiled=True)
        density.append(gather_groups(swapped[: members // 2], swapped[members // 2 :], groups))
    scaled = []
    for chunk in range(CHUNKS):
        sums = partial_crossings(core, trial_vectors, density[chunk], members, rows)
        given = flip(sums[1], "band", members, 1)
        on_chip = (sums[0].astype(jnp.float32) + given.astype(jnp.float32)).astype(jnp.bfloat16)
        along = lax.all_to_all(
            on_chip, "band", split_axis=0, concat_axis=0, tiled=True, axis_index_groups=lines
        )
        total = jnp.sum(along.astype(jnp.float32), 0)
        factor = own_weights[:, chunk * width : (chunk + 1) * width].reshape(1, 1, width)
        value = (factor * total).astype(jnp.bfloat16)
        copies = jnp.broadcast_to(value[None], (members // 2,) + value.shape)
        own = lax.all_to_all(
            copies, "band", split_axis=0, concat_axis=0, tiled=True, axis_index_groups=lines
        )
        scaled.append((own, flip(own, "band", members, 1)))
    images, subspace = make_images(
        core, weights, scaled, density, freqs, vecs, rows, groups, grid_count
    )
    return (images, subspace)


def solution(mesh):
    return jax.shard_map(
        shards,
        mesh=mesh,
        in_specs=(
            P(("freq", "band"), None, None),
            P("freq", None, None, "band"),
            P("freq"),
            P(),
            P(),
            P(("freq", "band")),
        ),
        out_specs=(P("freq", None, None, "band"), P("freq", None, None, None)),
        check_vma=False,
    )
```

```python
import functools
import math

import jax
import jax.numpy as jnp
from jax import lax
from jax.experimental import pallas as pl
from jax.experimental.pallas import tpu as pltpu
from jax.sharding import PartitionSpec as P

VMEM = pltpu.VMEM
ROWS_BY_ROWS = (((1,), (1,)), ((), ()))


def split_kernel(me_ref, density_ref, *out_refs):
    rows = density_ref.shape[0]
    block = density_ref[...].astype(jnp.float32)
    for n, out_ref in enumerate(out_refs):

        @pl.when(pl.program_id(0) == n)
        def _():
            for part in range(2):
                out_ref[part * rows : (part + 1) * rows, :] = block[:, part, :].astype(jnp.bfloat16)


def split_density(me, pair_density, members, line):
    stored, _, grid_all = pair_density.shape
    grid_own = grid_all // members
    shape = (2 * stored, grid_own)
    return pl.pallas_call(
        split_kernel,
        grid_spec=pltpu.PrefetchScalarGridSpec(
            num_scalar_prefetch=1,
            grid=(2,),
            in_specs=[
                pl.BlockSpec((stored, 2, grid_own), lambda n, me_ref: (0, 0, me_ref[0] ^ (2 * line + n)))
            ],
            out_specs=[pl.BlockSpec(shape, lambda n, me_ref: (0, 0))] * 2,
        ),
        out_shape=[jax.ShapeDtypeStruct(shape, jnp.bfloat16)] * 2,
        name="split_density",
    )(me, pair_density)


def flip(value, axis, size, mask):
    return lax.ppermute(value, axis, [(i, i ^ mask) for i in range(size)])


def gather_groups(block, groups, high_first):
    parts = {0: block}
    for mask in range(1, groups):
        bit = 1 << (mask.bit_length() - 1) if high_first else mask & -mask
        parts[mask] = flip(parts[mask ^ bit], "freq", groups, bit)
    return [parts[mask] for mask in range(groups)]


def crossing_kernel(groups, members, me_ref, vectors_ref, *refs):
    density_refs = refs[: groups * members]
    sorted_ref, keep_ref, give_ref = refs[groups * members :]
    freqs, _, vecs, grid_own = vectors_ref.shape
    rows = sorted_ref.shape[2] // members
    share = keep_ref.shape[2]
    pieces = vecs // share
    me = me_ref[0]
    north = me % 2 == 0
    vectors = vectors_ref[...].reshape(freqs * 2 * vecs, grid_own)
    for group in range(groups):
        for offset in range(members):
            start = pl.multiple_of((me ^ offset) * rows, rows)
            for part in range(2):
                sorted_ref[part, group, pl.ds(start, rows), :] = density_refs[group * members + offset][
                    part * rows : (part + 1) * rows, :
                ]
        width = members * rows
        columns = slice(group * width, (group + 1) * width)
        products = []
        for part in range(2):
            product = lax.dot_general(
                vectors, sorted_ref[part, group], ROWS_BY_ROWS, preferred_element_type=jnp.float32
            )
            products.append(product.reshape(freqs, 2, vecs, width))
        terms = (
            products[0][:, 0] + products[1][:, 1],
            products[0][:, 1] - products[1][:, 0],
        )
        for line in range(members // 2):
            target = line ^ (me // 2)
            for part in range(2):
                values = []
                for member in (2 * line, 2 * line + 1):
                    f, piece = member // pieces, member % pieces
                    values.append(terms[part][f, piece * share : (piece + 1) * share])
                keep_ref[target, part, :, columns] = jnp.where(north, values[0], values[1]).astype(jnp.bfloat16)
                give_ref[target, part, :, columns] = jnp.where(north, values[1], values[0]).astype(jnp.bfloat16)


def partial_crossings(me, vectors, density, members, stored):
    groups = len(density)
    freqs, _, vecs, grid_own = vectors.shape
    share = freqs * vecs // members
    width = members * stored * groups
    flat = [block for blocks in density for block in blocks]
    whole = pl.BlockSpec(memory_space=VMEM)
    part_shape = jax.ShapeDtypeStruct((members // 2, 2, share, width), jnp.bfloat16)
    return pl.pallas_call(
        functools.partial(crossing_kernel, groups, members),
        in_specs=[pl.BlockSpec(memory_space=pltpu.SMEM)] + [whole] * (1 + len(flat)),
        out_specs=[whole] * 3,
        out_shape=[
            jax.ShapeDtypeStruct((2, groups, members * stored, grid_own), jnp.bfloat16),
            part_shape,
            part_shape,
        ],
        cost_estimate=pl.CostEstimate(
            flops=8 * freqs * vecs * grid_own * width, bytes_accessed=8 * grid_own * width, transcendentals=0
        ),
        name="partial_crossings",
    )(me, vectors, *flat)


def image_kernel(chunks, members, grid_count, me_ref, weights_ref, *refs):
    scaled_refs, refs = refs[: chunks * members], refs[chunks * members :]
    density_refs = refs[:chunks]
    images_ref, subspace_ref, scaled_scr = refs[chunks:]
    freqs, _, vecs, _ = images_ref.shape
    share = scaled_refs[0].shape[1]
    pieces = vecs // share

    @pl.when(pl.program_id(0) == 0)
    def _():
        me = me_ref[0]
        begin = 0
        for chunk in range(chunks):
            width = scaled_refs[chunk * members].shape[2]
            for offset in range(members):
                member = me ^ offset
                f, piece = member // pieces, member % pieces
                for part in range(2):
                    scaled_scr[(f * 2 + part) * pieces + piece, :, begin : begin + width] = scaled_refs[
                        chunk * members + offset
                    ][part]
            begin += width
        for f in range(freqs):
            rows_f = scaled_scr[f * 2 * pieces : (f + 1) * 2 * pieces].reshape(2 * vecs, begin)
            ratio = rows_f.astype(jnp.float32) / weights_ref[f : f + 1, :]
            high = ratio.astype(jnp.bfloat16)
            low = (ratio - high.astype(jnp.float32)).astype(jnp.bfloat16)
            gram = lax.dot_general(high, rows_f, ROWS_BY_ROWS, preferred_element_type=jnp.float32)
            gram += lax.dot_general(low, rows_f, ROWS_BY_ROWS, preferred_element_type=jnp.float32)
            gram = gram * (1.0 / grid_count)
            subspace_ref[f, 0] = gram[:vecs, :vecs] + gram[vecs:, vecs:]
            subspace_ref[f, 1] = gram[:vecs, vecs:] - gram[vecs:, :vecs]

    scaled = scaled_scr[...].reshape(freqs * 2 * vecs, scaled_scr.shape[2])
    products = []
    for part in range(2):
        density = jnp.concatenate(
            [ref[part].reshape(ref.shape[1] * ref.shape[2], ref.shape[3]) for ref in density_refs], 0
        )
        product = jnp.dot(scaled, density, preferred_element_type=jnp.float32)
        products.append(product.reshape(freqs, 2, vecs, product.shape[1]))
    images_ref[:, 0] = products[0][:, 0] - products[1][:, 1]
    images_ref[:, 1] = products[0][:, 1] + products[1][:, 0]


def make_images(me, weights, scaled, density, freqs, vecs, members, grid_count):
    flat_scaled = [block for blocks in scaled for block in blocks]
    share = flat_scaled[0].shape[1]
    grid_own = density[0].shape[3]
    tile = math.gcd(grid_own, 256)
    total = weights.shape[1]
    whole = pl.BlockSpec(memory_space=VMEM)
    return pl.pallas_call(
        functools.partial(image_kernel, len(density), members, grid_count),
        grid=(grid_own // tile,),
        in_specs=[pl.BlockSpec(memory_space=pltpu.SMEM), whole]
        + [whole] * len(flat_scaled)
        + [pl.BlockSpec(block.shape[:3] + (tile,), lambda t: (0, 0, 0, t)) for block in density],
        out_specs=[
            pl.BlockSpec((freqs, 2, vecs, tile), lambda t: (0, 0, 0, t)),
            pl.BlockSpec((freqs, 2, vecs, vecs), lambda t: (0, 0, 0, 0)),
        ],
        out_shape=[
            jax.ShapeDtypeStruct((freqs, 2, vecs, grid_own), jnp.float32),
            jax.ShapeDtypeStruct((freqs, 2, vecs, vecs), jnp.float32),
        ],
        scratch_shapes=[VMEM((freqs * 2 * (vecs // share), share, total), jnp.bfloat16)],
        name="make_images",
    )(me, weights, *flat_scaled, *density)


def pair_weights(pair_index, frequency, val_energy, cond_energy, prefactor):
    cond_count = cond_energy.shape[0]
    val_count = val_energy.shape[0]
    cond_pick = jnp.sum(
        jnp.where(
            jnp.arange(cond_count)[:, None] == (pair_index % cond_count)[None, :], cond_energy[:, None], 0.0
        ),
        axis=0,
    )
    val_pick = jnp.sum(
        jnp.where(
            jnp.arange(val_count)[:, None] == (pair_index // cond_count)[None, :], val_energy[:, None], 0.0
        ),
        axis=0,
    )
    delta = cond_pick - val_pick
    ratio = delta[None, :] / (
        delta[None, :] * delta[None, :] + frequency[:, None] * frequency[:, None]
    )
    return lax.reduce_precision(-4.0 * prefactor * ratio, 8, 7)


def all_pair_numbers(pair_index, groups, members):
    me = lax.axis_index("band")
    slots = jnp.where(jnp.arange(members)[:, None] == me, pair_index[None, :], 0)
    mask = 1
    while mask < members:
        slots = slots + flip(slots, "band", members, mask)
        mask *= 2
    parts = [slots] + [flip(slots, "freq", groups, mask) for mask in range(1, groups)]
    return jnp.concatenate([part.reshape(-1) for part in parts])


def shards(pair_density, trial_vectors, frequency, val_energy, cond_energy, pair_index):
    groups = lax.axis_size("freq")
    members = lax.axis_size("band")
    lines = members // 2
    stored = pair_density.shape[0]
    freqs, _, vecs, grid_own = trial_vectors.shape
    pair_count = stored * groups * members
    grid_count = grid_own * members
    prefactor = 1.0 / math.sqrt(2.0 * grid_count * pair_count)
    pieces = members // freqs
    block = members * stored
    index = lax.axis_index("band").astype(jnp.int32)
    me = index.reshape(1)

    gathered = []
    for line in range(lines):
        for core, packed in enumerate(split_density(me, pair_density, members, line)):
            if line == 0 and core == 1:
                packed, pair_index = lax.optimization_barrier((packed, pair_index))
            offset = 2 * line + core
            arrived = flip(packed, "band", members, offset) if offset else packed
            gathered.append(gather_groups(arrived, groups, core == 0))
    numbers = all_pair_numbers(pair_index, groups, members)
    weights = pair_weights(numbers, frequency, val_energy, cond_energy, prefactor)
    own_weights = lax.dynamic_slice_in_dim(weights, index // pieces, 1, 0)

    scaled, density = [], []
    for first, last in ((0, groups - 1), (groups - 1, groups)):
        blocks = [[gathered[offset][group] for offset in range(members)] for group in range(first, last)]
        ordered, keep, give = partial_crossings(me, trial_vectors, blocks, members, stored)
        density.append(ordered)
        given = flip(give, "band", members, 1)
        total = keep[0].astype(jnp.float32) + given[0].astype(jnp.float32)
        for line in range(1, lines):
            on_chip = (keep[line].astype(jnp.float32) + given[line].astype(jnp.float32)).astype(jnp.bfloat16)
            total += flip(on_chip, "band", members, 2 * line).astype(jnp.float32)
        factor = own_weights[:, first * block : last * block].reshape(1, 1, (last - first) * block)
        value = (factor * total).astype(jnp.bfloat16)
        parts = []
        for line in range(lines):
            along = flip(value, "band", members, 2 * line) if line else value
            parts += [along, flip(along, "band", members, 1)]
        scaled.append(parts)
    images, subspace = make_images(me, weights, scaled, density, freqs, vecs, members, grid_count)
    return (images, subspace)


def solution(mesh):
    return jax.shard_map(
        shards,
        mesh=mesh,
        in_specs=(
            P(("freq", "band"), None, None),
            P("freq", None, None, "band"),
            P("freq"),
            P(),
            P(),
            P(("freq", "band")),
        ),
        out_specs=(P("freq", None, None, "band"), P("freq", None, None, None)),
        check_vma=False,
    )
```

```python
import functools
import math

import jax
import jax.numpy as jnp
from jax import lax
from jax.experimental import pallas as pl
from jax.experimental.pallas import tpu as pltpu
from jax.sharding import PartitionSpec as P

VMEM = pltpu.VMEM
ROWS_BY_ROWS = (((1,), (1,)), ((), ()))


def split_kernel(me_ref, density_ref, *out_refs):
    rows = density_ref.shape[0]
    block = density_ref[...].astype(jnp.float32)
    for n, out_ref in enumerate(out_refs):

        @pl.when(pl.program_id(0) == n)
        def _():
            for part in range(2):
                out_ref[part * rows : (part + 1) * rows, :] = block[:, part, :].astype(jnp.bfloat16)


def split_density(me, pair_density, members, line):
    stored, _, grid_all = pair_density.shape
    grid_own = grid_all // members
    shape = (2 * stored, grid_own)
    return pl.pallas_call(
        split_kernel,
        grid_spec=pltpu.PrefetchScalarGridSpec(
            num_scalar_prefetch=1,
            grid=(2,),
            in_specs=[
                pl.BlockSpec((stored, 2, grid_own), lambda n, me_ref: (0, 0, me_ref[0] ^ (2 * line + n)))
            ],
            out_specs=[pl.BlockSpec(shape, lambda n, me_ref: (0, 0))] * 2,
        ),
        out_shape=[jax.ShapeDtypeStruct(shape, jnp.bfloat16)] * 2,
        name="split_density",
    )(me, pair_density)


def flip(value, axis, size, mask):
    return lax.ppermute(value, axis, [(i, i ^ mask) for i in range(size)])


def gather_groups(block, groups, high_first):
    parts = {0: block}
    for mask in range(1, groups):
        bit = 1 << (mask.bit_length() - 1) if high_first else mask & -mask
        parts[mask] = flip(parts[mask ^ bit], "freq", groups, bit)
    return [parts[mask] for mask in range(groups)]


def crossing_kernel(groups, members, me_ref, vectors_ref, *refs):
    density_refs = refs[: groups * members]
    sorted_ref, keep_ref, give_ref = refs[groups * members :]
    freqs, _, vecs, grid_own = vectors_ref.shape
    rows = sorted_ref.shape[2] // members
    share = keep_ref.shape[2]
    pieces = vecs // share
    me = me_ref[0]
    north = me % 2 == 0
    vectors = vectors_ref[...].reshape(freqs * 2 * vecs, grid_own)
    for group in range(groups):
        for offset in range(members):
            start = pl.multiple_of((me ^ offset) * rows, rows)
            for part in range(2):
                sorted_ref[part, group, pl.ds(start, rows), :] = density_refs[group * members + offset][
                    part * rows : (part + 1) * rows, :
                ]
        width = members * rows
        columns = slice(group * width, (group + 1) * width)
        products = []
        for part in range(2):
            product = lax.dot_general(
                vectors, sorted_ref[part, group], ROWS_BY_ROWS, preferred_element_type=jnp.float32
            )
            products.append(product.reshape(freqs, 2, vecs, width))
        terms = (
            products[0][:, 0] + products[1][:, 1],
            products[0][:, 1] - products[1][:, 0],
        )
        for line in range(members // 2):
            target = line ^ (me // 2)
            for part in range(2):
                values = []
                for member in (2 * line, 2 * line + 1):
                    f, piece = member // pieces, member % pieces
                    values.append(terms[part][f, piece * share : (piece + 1) * share])
                keep_ref[target, part, :, columns] = jnp.where(north, values[0], values[1]).astype(jnp.bfloat16)
                give_ref[target, part, :, columns] = jnp.where(north, values[1], values[0]).astype(jnp.bfloat16)


def partial_crossings(me, vectors, density, members, stored):
    groups = len(density)
    freqs, _, vecs, grid_own = vectors.shape
    share = freqs * vecs // members
    width = members * stored * groups
    flat = [block for blocks in density for block in blocks]
    whole = pl.BlockSpec(memory_space=VMEM)
    part_shape = jax.ShapeDtypeStruct((members // 2, 2, share, width), jnp.bfloat16)
    return pl.pallas_call(
        functools.partial(crossing_kernel, groups, members),
        in_specs=[pl.BlockSpec(memory_space=pltpu.SMEM)] + [whole] * (1 + len(flat)),
        out_specs=[whole] * 3,
        out_shape=[
            jax.ShapeDtypeStruct((2, groups, members * stored, grid_own), jnp.bfloat16),
            part_shape,
            part_shape,
        ],
        cost_estimate=pl.CostEstimate(
            flops=8 * freqs * vecs * grid_own * width, bytes_accessed=8 * grid_own * width, transcendentals=0
        ),
        name="partial_crossings",
    )(me, vectors, *flat)


def image_kernel(chunks, members, grid_count, me_ref, weights_ref, *refs):
    scaled_refs, refs = refs[: chunks * members], refs[chunks * members :]
    density_refs = refs[:chunks]
    images_ref, subspace_ref, scaled_scr = refs[chunks:]
    freqs, _, vecs, _ = images_ref.shape
    share = scaled_refs[0].shape[1]
    pieces = vecs // share

    @pl.when(pl.program_id(0) == 0)
    def _():
        me = me_ref[0]
        begin = 0
        for chunk in range(chunks):
            width = scaled_refs[chunk * members].shape[2]
            for offset in range(members):
                member = me ^ offset
                f, piece = member // pieces, member % pieces
                for part in range(2):
                    scaled_scr[(f * 2 + part) * pieces + piece, :, begin : begin + width] = scaled_refs[
                        chunk * members + offset
                    ][part]
            begin += width
        for f in range(freqs):
            rows_f = scaled_scr[f * 2 * pieces : (f + 1) * 2 * pieces].reshape(2 * vecs, begin)
            ratio = rows_f.astype(jnp.float32) / weights_ref[f : f + 1, :]
            high = ratio.astype(jnp.bfloat16)
            low = (ratio - high.astype(jnp.float32)).astype(jnp.bfloat16)
            gram = lax.dot_general(high, rows_f, ROWS_BY_ROWS, preferred_element_type=jnp.float32)
            gram += lax.dot_general(low, rows_f, ROWS_BY_ROWS, preferred_element_type=jnp.float32)
            gram = gram * (1.0 / grid_count)
            subspace_ref[f, 0] = gram[:vecs, :vecs] + gram[vecs:, vecs:]
            subspace_ref[f, 1] = gram[:vecs, vecs:] - gram[vecs:, :vecs]

    scaled = scaled_scr[...].reshape(freqs * 2 * vecs, scaled_scr.shape[2])
    products = []
    for part in range(2):
        density = jnp.concatenate(
            [ref[part].reshape(ref.shape[1] * ref.shape[2], ref.shape[3]) for ref in density_refs], 0
        )
        product = jnp.dot(scaled, density, preferred_element_type=jnp.float32)
        products.append(product.reshape(freqs, 2, vecs, product.shape[1]))
    images_ref[:, 0] = products[0][:, 0] - products[1][:, 1]
    images_ref[:, 1] = products[0][:, 1] + products[1][:, 0]


def make_images(me, weights, scaled, density, freqs, vecs, members, grid_count):
    flat_scaled = [block for blocks in scaled for block in blocks]
    share = flat_scaled[0].shape[1]
    grid_own = density[0].shape[3]
    tile = math.gcd(grid_own, 256)
    total = weights.shape[1]
    whole = pl.BlockSpec(memory_space=VMEM)
    return pl.pallas_call(
        functools.partial(image_kernel, len(density), members, grid_count),
        grid=(grid_own // tile,),
        in_specs=[pl.BlockSpec(memory_space=pltpu.SMEM), whole]
        + [whole] * len(flat_scaled)
        + [pl.BlockSpec(block.shape[:3] + (tile,), lambda t: (0, 0, 0, t)) for block in density],
        out_specs=[
            pl.BlockSpec((freqs, 2, vecs, tile), lambda t: (0, 0, 0, t)),
            pl.BlockSpec((freqs, 2, vecs, vecs), lambda t: (0, 0, 0, 0)),
        ],
        out_shape=[
            jax.ShapeDtypeStruct((freqs, 2, vecs, grid_own), jnp.float32),
            jax.ShapeDtypeStruct((freqs, 2, vecs, vecs), jnp.float32),
        ],
        scratch_shapes=[VMEM((freqs * 2 * (vecs // share), share, total), jnp.bfloat16)],
        name="make_images",
    )(me, weights, *flat_scaled, *density)


def pair_weights(pair_index, frequency, val_energy, cond_energy, prefactor):
    cond_count = cond_energy.shape[0]
    val_count = val_energy.shape[0]
    cond_pick = jnp.sum(
        jnp.where(
            jnp.arange(cond_count)[:, None] == (pair_index % cond_count)[None, :], cond_energy[:, None], 0.0
        ),
        axis=0,
    )
    val_pick = jnp.sum(
        jnp.where(
            jnp.arange(val_count)[:, None] == (pair_index // cond_count)[None, :], val_energy[:, None], 0.0
        ),
        axis=0,
    )
    delta = cond_pick - val_pick
    ratio = delta[None, :] / (
        delta[None, :] * delta[None, :] + frequency[:, None] * frequency[:, None]
    )
    return lax.reduce_precision(-4.0 * prefactor * ratio, 8, 7)


def shards(pair_density, trial_vectors, frequency, val_energy, cond_energy, pair_index):
    groups = lax.axis_size("freq")
    members = lax.axis_size("band")
    lines = members // 2
    stored = pair_density.shape[0]
    freqs, _, vecs, grid_own = trial_vectors.shape
    pair_count = stored * groups * members
    grid_count = grid_own * members
    prefactor = 1.0 / math.sqrt(2.0 * grid_count * pair_count)
    pieces = members // freqs
    block = members * stored
    index = lax.axis_index("band").astype(jnp.int32)
    me = index.reshape(1)

    slots = jnp.where(jnp.arange(members)[:, None] == index, pair_index[None, :], 0)
    steps = [1 << bit for bit in range((members - 1).bit_length())]
    gathered = []
    for line in range(lines):
        for core, packed in enumerate(split_density(me, pair_density, members, line)):
            offset = 2 * line + core
            if offset == 1:
                packed, slots = lax.optimization_barrier((packed, slots))
                slots = slots + flip(slots, "band", members, steps.pop(0))
            arrived = flip(packed, "band", members, offset) if offset else packed
            if len(steps) > 1 and offset == 2 * line + 1 and line:
                arrived, slots = lax.optimization_barrier((arrived, slots))
                slots = slots + flip(slots, "band", members, steps.pop(0))
            elif offset == members - 1:
                for step in steps:
                    arrived, slots = lax.optimization_barrier((arrived, slots))
                    slots = slots + flip(slots, "band", members, step)
            gathered.append(gather_groups(arrived, groups, core == 0))
    gathered[-1][groups - 2], slots = lax.optimization_barrier((gathered[-1][groups - 2], slots))
    parts = [slots] + [flip(slots, "freq", groups, mask) for mask in range(1, groups)]
    numbers = jnp.concatenate([part.reshape(-1) for part in parts])
    weights = pair_weights(numbers, frequency, val_energy, cond_energy, prefactor)
    own_weights = lax.dynamic_slice_in_dim(weights, index // pieces, 1, 0)

    scaled, density = [], []
    for first, last in ((0, groups - 1), (groups - 1, groups)):
        blocks = [[gathered[offset][group] for offset in range(members)] for group in range(first, last)]
        ordered, keep, give = partial_crossings(me, trial_vectors, blocks, members, stored)
        density.append(ordered)
        given = flip(give, "band", members, 1)
        total = keep[0].astype(jnp.float32) + given[0].astype(jnp.float32)
        for line in range(1, lines):
            on_chip = (keep[line].astype(jnp.float32) + given[line].astype(jnp.float32)).astype(jnp.bfloat16)
            total += flip(on_chip, "band", members, 2 * line).astype(jnp.float32)
        factor = own_weights[:, first * block : last * block].reshape(1, 1, (last - first) * block)
        value = (factor * total).astype(jnp.bfloat16)
        parts = []
        for line in range(lines):
            along = flip(value, "band", members, 2 * line) if line else value
            if last == groups:
                parts += [along, flip(value, "band", members, 2 * line + 1)]
            else:
                parts += [along, flip(along, "band", members, 1)]
        scaled.append(parts)
    images, subspace = make_images(me, weights, scaled, density, freqs, vecs, members, grid_count)
    return (images, subspace)


def solution(mesh):
    return jax.shard_map(
        shards,
        mesh=mesh,
        in_specs=(
            P(("freq", "band"), None, None),
            P("freq", None, None, "band"),
            P("freq"),
            P(),
            P(),
            P(("freq", "band")),
        ),
        out_specs=(P("freq", None, None, "band"), P("freq", None, None, None)),
        check_vma=False,
    )
```

```python
import functools
import math

import jax
import jax.numpy as jnp
from jax import lax
from jax.experimental import pallas as pl
from jax.experimental.pallas import tpu as pltpu
from jax.sharding import PartitionSpec as P

VMEM = pltpu.VMEM
ROWS_BY_ROWS = (((1,), (1,)), ((), ()))


def split_kernel(me_ref, density_ref, *out_refs):
    rows = density_ref.shape[0]
    block = density_ref[...].astype(jnp.float32)
    for n, out_ref in enumerate(out_refs):

        @pl.when(pl.program_id(0) == n)
        def _():
            for part in range(2):
                out_ref[part * rows : (part + 1) * rows, :] = block[:, part, :].astype(jnp.bfloat16)


def split_density(me, pair_density, members, line):
    stored, _, grid_all = pair_density.shape
    grid_own = grid_all // members
    shape = (2 * stored, grid_own)
    return pl.pallas_call(
        split_kernel,
        grid_spec=pltpu.PrefetchScalarGridSpec(
            num_scalar_prefetch=1,
            grid=(2,),
            in_specs=[
                pl.BlockSpec((stored, 2, grid_own), lambda n, me_ref: (0, 0, me_ref[0] ^ (2 * line + n)))
            ],
            out_specs=[pl.BlockSpec(shape, lambda n, me_ref: (0, 0))] * 2,
        ),
        out_shape=[jax.ShapeDtypeStruct(shape, jnp.bfloat16)] * 2,
        name="split_density",
    )(me, pair_density)


def flip(value, axis, size, mask):
    return lax.ppermute(value, axis, [(i, i ^ mask) for i in range(size)])


def gather_groups(block, groups, high_first):
    parts = {0: block}
    for mask in range(1, groups):
        bit = 1 << (mask.bit_length() - 1) if high_first else mask & -mask
        parts[mask] = flip(parts[mask ^ bit], "freq", groups, bit)
    return [parts[mask] for mask in range(groups)]


def crossing_kernel(groups, members, me_ref, vectors_ref, *refs):
    lines = members // 2
    density_refs = refs[: groups * lines]
    sorted_ref, keep_ref, give_ref = refs[groups * lines :]
    freqs, _, vecs, grid_own = vectors_ref.shape
    rows = sorted_ref.shape[2] // members
    share = keep_ref.shape[2]
    pieces = vecs // share
    me = me_ref[0]
    north = me % 2 == 0
    vectors = vectors_ref[...].reshape(freqs * 2 * vecs, grid_own)
    for group in range(groups):
        for offset in range(members):
            start = pl.multiple_of((me ^ offset) * rows, rows)
            for part in range(2):
                begin = (2 * (offset % 2) + part) * rows
                sorted_ref[part, group, pl.ds(start, rows), :] = density_refs[group * lines + offset // 2][
                    begin : begin + rows, :
                ]
        width = members * rows
        columns = slice(group * width, (group + 1) * width)
        products = []
        for part in range(2):
            product = lax.dot_general(
                vectors, sorted_ref[part, group], ROWS_BY_ROWS, preferred_element_type=jnp.float32
            )
            products.append(product.reshape(freqs, 2, vecs, width))
        terms = (
            products[0][:, 0] + products[1][:, 1],
            products[0][:, 1] - products[1][:, 0],
        )
        for line in range(members // 2):
            target = line ^ (me // 2)
            for part in range(2):
                values = []
                for member in (2 * line, 2 * line + 1):
                    f, piece = member // pieces, member % pieces
                    values.append(terms[part][f, piece * share : (piece + 1) * share])
                keep_ref[target, part, :, columns] = jnp.where(north, values[0], values[1]).astype(jnp.bfloat16)
                give_ref[target, part, :, columns] = jnp.where(north, values[1], values[0]).astype(jnp.bfloat16)


def partial_crossings(me, vectors, density, members, stored):
    groups = len(density)
    freqs, _, vecs, grid_own = vectors.shape
    share = freqs * vecs // members
    width = members * stored * groups
    flat = [block for blocks in density for block in blocks]
    whole = pl.BlockSpec(memory_space=VMEM)
    part_shape = jax.ShapeDtypeStruct((members // 2, 2, share, width), jnp.bfloat16)
    return pl.pallas_call(
        functools.partial(crossing_kernel, groups, members),
        in_specs=[pl.BlockSpec(memory_space=pltpu.SMEM)] + [whole] * (1 + len(flat)),
        out_specs=[whole] * 3,
        out_shape=[
            jax.ShapeDtypeStruct((2, groups, members * stored, grid_own), jnp.bfloat16),
            part_shape,
            part_shape,
        ],
        cost_estimate=pl.CostEstimate(
            flops=8 * freqs * vecs * grid_own * width, bytes_accessed=8 * grid_own * width, transcendentals=0
        ),
        name="partial_crossings",
    )(me, vectors, *flat)


def image_kernel(chunks, members, grid_count, me_ref, weights_ref, *refs):
    scaled_refs, refs = refs[: chunks * members], refs[chunks * members :]
    density_refs = refs[:chunks]
    images_ref, subspace_ref, scaled_scr = refs[chunks:]
    freqs, _, vecs, _ = images_ref.shape
    share = scaled_refs[0].shape[1]
    pieces = vecs // share

    @pl.when(pl.program_id(0) == 0)
    def _():
        me = me_ref[0]
        begin = 0
        for chunk in range(chunks):
            width = scaled_refs[chunk * members].shape[2]
            for offset in range(members):
                member = me ^ offset
                f, piece = member // pieces, member % pieces
                for part in range(2):
                    scaled_scr[(f * 2 + part) * pieces + piece, :, begin : begin + width] = scaled_refs[
                        chunk * members + offset
                    ][part]
            begin += width
        for f in range(freqs):
            rows_f = scaled_scr[f * 2 * pieces : (f + 1) * 2 * pieces].reshape(2 * vecs, begin)
            ratio = rows_f.astype(jnp.float32) / weights_ref[f : f + 1, :]
            high = ratio.astype(jnp.bfloat16)
            low = (ratio - high.astype(jnp.float32)).astype(jnp.bfloat16)
            gram = lax.dot_general(high, rows_f, ROWS_BY_ROWS, preferred_element_type=jnp.float32)
            gram += lax.dot_general(low, rows_f, ROWS_BY_ROWS, preferred_element_type=jnp.float32)
            gram = gram * (1.0 / grid_count)
            subspace_ref[f, 0] = gram[:vecs, :vecs] + gram[vecs:, vecs:]
            subspace_ref[f, 1] = gram[:vecs, vecs:] - gram[vecs:, :vecs]

    scaled = scaled_scr[...].reshape(freqs * 2 * vecs, scaled_scr.shape[2])
    products = []
    for part in range(2):
        density = jnp.concatenate(
            [ref[part].reshape(ref.shape[1] * ref.shape[2], ref.shape[3]) for ref in density_refs], 0
        )
        product = jnp.dot(scaled, density, preferred_element_type=jnp.float32)
        products.append(product.reshape(freqs, 2, vecs, product.shape[1]))
    images_ref[:, 0] = products[0][:, 0] - products[1][:, 1]
    images_ref[:, 1] = products[0][:, 1] + products[1][:, 0]


def make_images(me, weights, scaled, density, freqs, vecs, members, grid_count):
    flat_scaled = [block for blocks in scaled for block in blocks]
    share = flat_scaled[0].shape[1]
    grid_own = density[0].shape[3]
    tile = math.gcd(grid_own, 256)
    total = weights.shape[1]
    whole = pl.BlockSpec(memory_space=VMEM)
    return pl.pallas_call(
        functools.partial(image_kernel, len(density), members, grid_count),
        grid=(grid_own // tile,),
        in_specs=[pl.BlockSpec(memory_space=pltpu.SMEM), whole]
        + [whole] * len(flat_scaled)
        + [pl.BlockSpec(block.shape[:3] + (tile,), lambda t: (0, 0, 0, t)) for block in density],
        out_specs=[
            pl.BlockSpec((freqs, 2, vecs, tile), lambda t: (0, 0, 0, t)),
            pl.BlockSpec((freqs, 2, vecs, vecs), lambda t: (0, 0, 0, 0)),
        ],
        out_shape=[
            jax.ShapeDtypeStruct((freqs, 2, vecs, grid_own), jnp.float32),
            jax.ShapeDtypeStruct((freqs, 2, vecs, vecs), jnp.float32),
        ],
        scratch_shapes=[VMEM((freqs * 2 * (vecs // share), share, total), jnp.bfloat16)],
        name="make_images",
    )(me, weights, *flat_scaled, *density)


def pair_weights(pair_index, frequency, val_energy, cond_energy, prefactor):
    cond_count = cond_energy.shape[0]
    val_count = val_energy.shape[0]
    cond_pick = jnp.sum(
        jnp.where(
            jnp.arange(cond_count)[:, None] == (pair_index % cond_count)[None, :], cond_energy[:, None], 0.0
        ),
        axis=0,
    )
    val_pick = jnp.sum(
        jnp.where(
            jnp.arange(val_count)[:, None] == (pair_index // cond_count)[None, :], val_energy[:, None], 0.0
        ),
        axis=0,
    )
    delta = cond_pick - val_pick
    ratio = delta[None, :] / (
        delta[None, :] * delta[None, :] + frequency[:, None] * frequency[:, None]
    )
    return lax.reduce_precision(-4.0 * prefactor * ratio, 8, 7)


def shards(pair_density, trial_vectors, frequency, val_energy, cond_energy, pair_index):
    groups = lax.axis_size("freq")
    members = lax.axis_size("band")
    lines = members // 2
    stored = pair_density.shape[0]
    freqs, _, vecs, grid_own = trial_vectors.shape
    pair_count = stored * groups * members
    grid_count = grid_own * members
    prefactor = 1.0 / math.sqrt(2.0 * grid_count * pair_count)
    pieces = members // freqs
    block = members * stored
    index = lax.axis_index("band").astype(jnp.int32)
    me = index.reshape(1)

    slots = jnp.where(jnp.arange(members)[:, None] == index, pair_index[None, :], 0)
    steps = [1 << bit for bit in range((members - 1).bit_length())]
    gathered = []
    for line in range(lines):
        couple = []
        for core, packed in enumerate(split_density(me, pair_density, members, line)):
            offset = 2 * line + core
            if offset == 1:
                packed, slots = lax.optimization_barrier((packed, slots))
                slots = slots + flip(slots, "band", members, steps.pop(0))
            arrived = flip(packed, "band", members, offset) if offset else packed
            if len(steps) > 1 and offset == 2 * line + 1 and line:
                arrived, slots = lax.optimization_barrier((arrived, slots))
                slots = slots + flip(slots, "band", members, steps.pop(0))
            elif offset == members - 1:
                for step in steps:
                    arrived, slots = lax.optimization_barrier((arrived, slots))
                    slots = slots + flip(slots, "band", members, step)
            couple.append(arrived)
        gathered.append(gather_groups(jnp.concatenate(couple, 0), groups, line % 2 == 0))
    gathered[-1][groups - 2], slots = lax.optimization_barrier((gathered[-1][groups - 2], slots))
    parts = [slots] + [flip(slots, "freq", groups, mask) for mask in range(1, groups)]
    numbers = jnp.concatenate([part.reshape(-1) for part in parts])
    weights = pair_weights(numbers, frequency, val_energy, cond_energy, prefactor)
    own_weights = lax.dynamic_slice_in_dim(weights, index // pieces, 1, 0)

    scaled, density = [], []
    for first, last in ((0, groups - 1), (groups - 1, groups)):
        blocks = [[blocks_of[group] for blocks_of in gathered] for group in range(first, last)]
        ordered, keep, give = partial_crossings(me, trial_vectors, blocks, members, stored)
        density.append(ordered)
        given = flip(give, "band", members, 1)
        total = keep[0].astype(jnp.float32) + given[0].astype(jnp.float32)
        for line in range(1, lines):
            on_chip = (keep[line].astype(jnp.float32) + given[line].astype(jnp.float32)).astype(jnp.bfloat16)
            total += flip(on_chip, "band", members, 2 * line).astype(jnp.float32)
        factor = own_weights[:, first * block : last * block].reshape(1, 1, (last - first) * block)
        value = (factor * total).astype(jnp.bfloat16)
        parts = []
        for line in range(lines):
            along = flip(value, "band", members, 2 * line) if line else value
            if last == groups:
                parts += [along, flip(value, "band", members, 2 * line + 1)]
            else:
                parts += [along, flip(along, "band", members, 1)]
        scaled.append(parts)
    images, subspace = make_images(me, weights, scaled, density, freqs, vecs, members, grid_count)
    return (images, subspace)


def solution(mesh):
    return jax.shard_map(
        shards,
        mesh=mesh,
        in_specs=(
            P(("freq", "band"), None, None),
            P("freq", None, None, "band"),
            P("freq"),
            P(),
            P(),
            P(("freq", "band")),
        ),
        out_specs=(P("freq", None, None, "band"), P("freq", None, None, None)),
        check_vma=False,
    )
```
